256 devices in a mesh: rows: 128 (over x, y, z), sub: 2 (over core).
Axes of the slice: x: 4, y: 4, z: 8, core: 2. Of those that a mesh axis runs over, the one named last changes fastest.
Arguments:
- tokens_x: bfloat16 [16384, 6144], P(('rows', 'sub')), may hold values from -24 to 24
- test_matrix: bfloat16 [96, 6144], replicated, may hold values from -0.078125 to 0.078125
Outputs:
- basis: float32 [16384, 96], P(('rows', 'sub'))
- projected: float32 [6144, 96], P(('rows', 'sub'))
The draws below stay inside these ranges and needn't reach their ends.
All inputs are finite; a program needn't handle non-finite values.
Results may differ from the reference program's by a relative error of at most 0.012.
The reference program's roundings to bfloat16 on the way (of `sketch` and `middle`) count: a program that leaves them out, or rounds other values in their place, can miss the bound.
Values may be sent and summed in bfloat16 or wider, within the bound.
No kernel may reach another device: no remote copies, remote signals or barrier semaphores. Data moves between devices by JAX's collectives and lax.ppermute only.
A program may use at most 64 MiB of HBM per device.

```python
import jax
import jax.numpy as jnp
from jax import lax

D = 6144
K = 96
TOKENS = 16384


def strengthened(entries, own_key, source, target, parts, factor):
    def block_of(dim):
        return (jnp.arange(entries.shape[dim]) // (entries.shape[dim] // parts)).reshape((-1,) + (1,) * (entries.ndim - 1 - dim))

    first = jax.random.permutation(own_key, parts)[block_of(target)]
    other_side = (block_of(target) + parts // 2) % parts
    return jnp.where((block_of(source) == first) | (block_of(source) == other_side), factor * entries, entries)


def level_of(key, extent, pieces, low, top_value):
    factor_of = 1.0
    for position, blocks in pieces:
        heights = jax.random.uniform(jax.random.fold_in(jax.random.fold_in(key, 6), position), (blocks,), jnp.float32, low / len(pieces), top_value / len(pieces))
        factor_of = factor_of * jnp.repeat(jnp.exp(heights), extent[position] // blocks).reshape((-1,) + (1,) * (len(extent) - 1 - position))
    return factor_of


def bell_draw(rng, extent, spread, most, pieces=(), held_as=jnp.bfloat16):
    values = spread * jax.random.normal(rng, extent, jnp.float32)
    if pieces:
        values = values * level_of(rng, extent, pieces, -0.22, 0.18)
    return jnp.clip(values, -most, most).astype(held_as)


def heavy_noise(key, extent, width, most, cuts, heavy, held_as=jnp.bfloat16):
    drawn = width * jax.random.normal(key, extent, jnp.float32)
    if cuts:
        drawn = drawn * level_of(key, extent, cuts, -0.22, 0.18)
    return jnp.clip(strengthened(drawn, jax.random.fold_in(key, 3), *heavy), -most, most).astype(held_as)


def setup_inputs(seed: int = 0) -> dict:
    seeds = jax.random.split(jax.random.key(seed), 3)
    tokens_x = heavy_noise(seeds[0], (TOKENS, D), 1.0, 24.0, ((0, 256),), (0, 1, 256, 6.0))
    test_matrix = bell_draw(seeds[1], (K, D), D ** -0.5, 0.078125)
    return {"tokens_x": tokens_x, "test_matrix": test_matrix}


def solve_right(factor, matrix):
    return lax.linalg.triangular_solve(factor, matrix, left_side=False, lower=True, transpose_a=True)

def symmetric(product, total):
    return (product + product.T) / (2.0 * total)

def reference(tokens_x, test_matrix):
    total = jnp.float32(tokens_x.shape[0])
    sketch = lax.dot_general(tokens_x.astype(jnp.float32), test_matrix.astype(jnp.float32), (((1,), (1,)), ((), ())), preferred_element_type=jnp.float32).astype(jnp.bfloat16)
    cross = lax.dot_general(tokens_x.astype(jnp.float32), sketch.astype(jnp.float32), (((0,), (0,)), ((), ())), preferred_element_type=jnp.float32)
    omega = test_matrix.astype(jnp.float32)
    gram_one = symmetric(jnp.dot(omega.astype(jnp.float32), cross.astype(jnp.float32), precision=lax.Precision.HIGHEST, preferred_element_type=jnp.float32), total)
    factor_one = jnp.linalg.cholesky(gram_one)
    middle = solve_right(factor_one, cross).astype(jnp.bfloat16)
    power = jnp.dot(tokens_x.astype(jnp.float32), middle.astype(jnp.float32), preferred_element_type=jnp.float32)
    cross_two = lax.dot_general(tokens_x.astype(jnp.float32), power.astype(jnp.bfloat16).astype(jnp.float32), (((0,), (0,)), ((), ())), preferred_element_type=jnp.float32)
    gram_two = symmetric(jnp.dot(middle.astype(jnp.float32).T.astype(jnp.float32), cross_two.astype(jnp.float32), precision=lax.Precision.HIGHEST, preferred_element_type=jnp.float32), total)
    factor_two = jnp.linalg.cholesky(gram_two)
    basis = solve_right(factor_two, power)
    projected = solve_right(factor_two, cross_two) / jnp.sqrt(total)
    return (basis, projected)
```

```python
import jax
import jax.numpy as jnp
from jax import lax
from jax.sharding import Mesh
from jax.sharding import PartitionSpec as P

PLANE = ("x", "y")
LINE = ("z", "core")
EVERY = ("x", "y", "z", "core")


def exchanged(array, axes):
    return lax.all_to_all(array, axes, 0, 0, tiled=True)


def from_everyone(array, axes):
    return exchanged(jnp.broadcast_to(array, (lax.axis_size(axes), *array.shape)), axes)


def solve_right(factor, matrix):
    return lax.linalg.triangular_solve(
        factor, matrix, left_side=False, lower=True, transpose_a=True
    )


def over_tokens(left, right):
    return lax.dot_general(
        left, right, (((0,), (0,)), ((), ())), preferred_element_type=jnp.float32
    )


def in_two(array):
    high = lax.reduce_precision(array, 8, 7)
    return high.astype(jnp.bfloat16), (array - high).astype(jnp.bfloat16)


def gram_of(high, low, total):
    product = over_tokens(high, high) + over_tokens(low, high)
    return (product + product.T) / (2.0 * total)


def on_device(tokens_x, test_matrix):
    rows, width = tokens_x.shape
    columns = test_matrix.shape[0]
    plane, line, pair = (lax.axis_size(a) for a in (PLANE, LINE, "core"))
    total = jnp.float32(rows * plane * line)
    block = width // plane
    share = block // line
    sketch = lax.dot_general(
        tokens_x, test_matrix, (((1,), (1,)), ((), ())), preferred_element_type=jnp.float32
    )
    high, low = in_two(sketch)
    blocks = jnp.swapaxes(tokens_x.reshape(rows, plane, block), 0, 1)
    both = jnp.broadcast_to(jnp.concatenate([high, low], 1), (plane, rows, 2 * columns))
    mixed = exchanged(jnp.concatenate([blocks, both], 2), PLANE).reshape(plane * rows, -1)
    tokens = mixed[:, :block]
    high = mixed[:, block : block + columns]
    low = mixed[:, block + columns :]
    gram = gram_of(high, low, total)
    cross = over_tokens(tokens, high)
    sent = jnp.concatenate(
        [cross.reshape(line, share, columns), gram.reshape(line, -1, columns)], 1
    )
    whole = from_everyone(jnp.sum(exchanged(sent, LINE), 0), LINE)
    cross = whole[:, :share].reshape(block, columns)
    gram_one = whole[:, share:].reshape(columns, columns)
    middle = solve_right(jnp.linalg.cholesky(gram_one), cross).astype(jnp.bfloat16)
    power = jnp.dot(tokens, middle, preferred_element_type=jnp.float32)
    power = jnp.sum(exchanged(power.reshape(plane, rows, columns), PLANE), 0)
    powers = from_everyone(power, PLANE).reshape(plane * rows, columns)
    high, low = in_two(powers)
    gram = gram_of(high, low, total)
    cross_two = over_tokens(tokens, high)
    halves = jnp.broadcast_to(
        gram.reshape(1, pair, -1, columns), (line // pair, pair, columns // pair, columns)
    )
    sent = jnp.concatenate(
        [cross_two.reshape(line, share, columns), halves.reshape(line, -1, columns)], 1
    )
    own = jnp.sum(exchanged(sent, LINE), 0)
    cross_two = own[:share]
    gram_two = lax.all_gather(own[share:], "core", axis=0, tiled=True)
    factor_two = jnp.linalg.cholesky(gram_two)
    basis = solve_right(factor_two, power)
    projected = solve_right(factor_two, cross_two) / jnp.sqrt(total)
    return (basis, projected)


def solution(mesh):
    finer = Mesh(mesh.devices.reshape(4, 4, 8, mesh.shape["sub"]), EVERY)
    return jax.shard_map(
        on_device,
        mesh=finer,
        in_specs=(P(EVERY, None), P()),
        out_specs=(P(EVERY, None), P(EVERY, None)),
        check_vma=False,
    )
```

```python
import jax
import jax.numpy as jnp
from jax import lax
from jax.experimental import pallas as pl
from jax.sharding import Mesh
from jax.sharding import PartitionSpec as P

PLANE = ("x", "y")
LINE = ("z", "core")
EVERY = ("x", "y", "z", "core")
GROUP = 8


def exchanged(array, axes):
    return lax.all_to_all(array, axes, 0, 0, tiled=True)


def from_everyone(array, axes):
    return exchanged(jnp.broadcast_to(array, (lax.axis_size(axes), *array.shape)), axes)


def inverse_factor_kernel(gram, inverse):
    size = gram.shape[0]
    shape = (GROUP, size)
    lane = lax.broadcasted_iota(jnp.int32, shape, 1)
    row = lax.broadcasted_iota(jnp.int32, shape, 0)

    def column(value, at):
        return jnp.broadcast_to(value[:, at : at + 1], shape)

    def line(value, at):
        return jnp.broadcast_to(value[at : at + 1], shape)

    groups = [gram[pl.ds(first, GROUP), :] for first in range(0, size, GROUP)]
    for at, own in enumerate(groups):
        first = at * GROUP
        columns = [column(own, first + k) for k in range(GROUP)]
        pivots = jnp.ones(shape, jnp.float32)
        lines, scales, uppers = [], [], {}
        for k in range(GROUP):
            pivot = line(columns[k], k)
            scale = 1.0 / pivot
            pivots = jnp.where(row == k, pivot, pivots)
            factor = jnp.where(row > k, columns[k] * scale, 0.0)
            own = jnp.where((lane == first + k) & (row >= k), jnp.where(row == k, 1.0, 0.0), own)
            lines.append(line(own, k))
            scales.append(scale)
            own = own - factor * lines[k]
            lines[k] = jnp.where((lane > first + k) & (lane < first + GROUP), 0.0, lines[k])
            for j in range(k + 1, GROUP):
                uppers[k, j] = line(columns[j], k)
                columns[j] = columns[j] - factor * uppers[k, j]
        inverse[pl.ds(first, GROUP), :] = jnp.where(
            lane <= first + row, own * lax.rsqrt(pivots), 0.0
        )
        inside = (lane >= first) & (lane < first + GROUP)
        for later in range(at + 1, len(groups)):
            value = groups[later]
            columns = [column(value, first + k) for k in range(GROUP)]
            value = jnp.where(inside, 0.0, value)
            for k in range(GROUP):
                factor = columns[k] * scales[k]
                value = value - factor * lines[k]
                for j in range(k + 1, GROUP):
                    columns[j] = columns[j] - factor * uppers[k, j]
            groups[later] = value

def inverse_factor(gram):
    return pl.pallas_call(
        inverse_factor_kernel, out_shape=jax.ShapeDtypeStruct(gram.shape, jnp.float32)
    )(gram)


def solved(matrix, inverse):
    return lax.dot_general(
        matrix,
        inverse,
        (((1,), (1,)), ((), ())),
        precision=lax.Precision.HIGHEST,
        preferred_element_type=jnp.float32,
    )


def over_tokens(left, right):
    return lax.dot_general(
        left, right, (((0,), (0,)), ((), ())), preferred_element_type=jnp.float32
    )


def in_two(array):
    high = lax.reduce_precision(array, 8, 7)
    return high.astype(jnp.bfloat16), (array - high).astype(jnp.bfloat16)


def gram_of(high, low, total):
    product = over_tokens(high, high) + over_tokens(low, high)
    return (product + product.T) / (2.0 * total)


def on_device(tokens_x, test_matrix):
    rows, width = tokens_x.shape
    columns = test_matrix.shape[0]
    plane, line, pair = (lax.axis_size(a) for a in (PLANE, LINE, "core"))
    total = jnp.float32(rows * plane * line)
    block = width // plane
    share = block // line
    sketch = lax.dot_general(
        tokens_x, test_matrix, (((1,), (1,)), ((), ())), preferred_element_type=jnp.float32
    )
    high, low = in_two(sketch)
    blocks = jnp.swapaxes(tokens_x.reshape(rows, plane, block), 0, 1)
    both = jnp.broadcast_to(jnp.concatenate([high, low], 1), (plane, rows, 2 * columns))
    mixed = exchanged(jnp.concatenate([blocks, both], 2), PLANE).reshape(plane * rows, -1)
    tokens = mixed[:, :block]
    high = mixed[:, block : block + columns]
    low = mixed[:, block + columns :]
    gram = gram_of(high, low, total)
    cross = over_tokens(tokens, high)
    part = columns // line
    sent = jnp.concatenate(
        [
            cross.reshape(line, share, columns),
            jnp.pad(gram.reshape(line, part, columns), ((0, 0), (0, GROUP - part), (0, 0))),
        ],
        1,
    )
    whole = from_everyone(jnp.sum(exchanged(sent, LINE), 0), LINE)
    cross = whole[:, :share].reshape(block, columns)
    gram_one = whole[:, share : share + part].reshape(columns, columns)
    middle = solved(cross, inverse_factor(gram_one)).astype(jnp.bfloat16)
    power = jnp.dot(tokens, middle, preferred_element_type=jnp.float32)
    power = jnp.sum(exchanged(power.reshape(plane, rows, columns), PLANE), 0)
    powers = from_everyone(power, PLANE).reshape(plane * rows, columns)
    high, low = in_two(powers)
    gram = gram_of(high, low, total)
    cross_two = over_tokens(tokens, high)
    halves = jnp.broadcast_to(
        gram.reshape(1, pair, -1, columns), (line // pair, pair, columns // pair, columns)
    )
    sent = jnp.concatenate(
        [cross_two.reshape(line, share, columns), halves.reshape(line, -1, columns)], 1
    )
    own = jnp.sum(exchanged(sent, LINE), 0)
    cross_two = own[:share]
    gram_two = lax.all_gather(own[share:], "core", axis=0, tiled=True)
    inverse_two = inverse_factor(gram_two)
    basis = solved(power, inverse_two)
    projected = solved(cross_two, inverse_two) / jnp.sqrt(total)
    return (basis, projected)


def solution(mesh):
    finer = Mesh(mesh.devices.reshape(4, 4, 8, mesh.shape["sub"]), EVERY)
    return jax.shard_map(
        on_device,
        mesh=finer,
        in_specs=(P(EVERY, None), P()),
        out_specs=(P(EVERY, None), P(EVERY, None)),
        check_vma=False,
    )
```

```python
import jax
import jax.numpy as jnp
from jax import lax
from jax.experimental import pallas as pl
from jax.sharding import Mesh
from jax.sharding import PartitionSpec as P

PLANE = ("x", "y")
LINE = ("z", "core")
EVERY = ("x", "y", "z", "core")
GROUP = 8
LANES = 128


def exchanged(array, axes):
    return lax.all_to_all(array, axes, 0, 0, tiled=True)


def from_everyone(array, axes):
    return exchanged(jnp.broadcast_to(array, (lax.axis_size(axes), *array.shape)), axes)


def inverse_factor_kernel(gram, inverse):
    size = gram.shape[0]
    shape = (GROUP, size)
    lane = lax.broadcasted_iota(jnp.int32, shape, 1)
    row = lax.broadcasted_iota(jnp.int32, shape, 0)

    def column(value, at):
        return jnp.broadcast_to(value[:, at : at + 1], shape)

    def line(value, at):
        return jnp.broadcast_to(value[at : at + 1], shape)

    groups = [gram[pl.ds(first, GROUP), :] for first in range(0, size, GROUP)]
    for at, own in enumerate(groups):
        first = at * GROUP
        columns = [column(own, first + k) for k in range(GROUP)]
        pivots = jnp.ones(shape, jnp.float32)
        lines, scales, uppers = [], [], {}
        for k in range(GROUP):
            pivot = line(columns[k], k)
            scale = 1.0 / pivot
            pivots = jnp.where(row == k, pivot, pivots)
            factor = jnp.where(row > k, columns[k] * scale, 0.0)
            own = jnp.where((lane == first + k) & (row >= k), jnp.where(row == k, 1.0, 0.0), own)
            lines.append(line(own, k))
            scales.append(scale)
            own = own - factor * lines[k]
            lines[k] = jnp.where((lane > first + k) & (lane < first + GROUP), 0.0, lines[k])
            for j in range(k + 1, GROUP):
                uppers[k, j] = line(columns[j], k)
                columns[j] = columns[j] - factor * uppers[k, j]
        inverse[pl.ds(first, GROUP), :] = jnp.where(
            lane <= first + row, own * lax.rsqrt(pivots), 0.0
        )
        inside = (lane >= first) & (lane < first + GROUP)
        for later in range(at + 1, len(groups)):
            value = groups[later]
            columns = [column(value, first + k) for k in range(GROUP)]
            value = jnp.where(inside, 0.0, value)
            for k in range(GROUP):
                factor = columns[k] * scales[k]
                value = value - factor * lines[k]
                for j in range(k + 1, GROUP):
                    columns[j] = columns[j] - factor * uppers[k, j]
            groups[later] = value

def inverse_factor(gram):
    return pl.pallas_call(
        inverse_factor_kernel, out_shape=jax.ShapeDtypeStruct(gram.shape, jnp.float32)
    )(gram)


def solved(matrix, inverse):
    return lax.dot_general(
        matrix,
        inverse,
        (((1,), (1,)), ((), ())),
        precision=lax.Precision.HIGHEST,
        preferred_element_type=jnp.float32,
    )


def over_tokens(left, right):
    return lax.dot_general(
        left, right, (((0,), (0,)), ((), ())), preferred_element_type=jnp.float32
    )


def in_two(array):
    high = lax.reduce_precision(array, 8, 7)
    return high.astype(jnp.bfloat16), (array - high).astype(jnp.bfloat16)


def gram_of(high, low, total):
    product = over_tokens(high, high) + over_tokens(low, high)
    return (product + product.T) / (2.0 * total)


def on_device(tokens_x, test_matrix):
    rows, width = tokens_x.shape
    columns = test_matrix.shape[0]
    plane, line, pair = (lax.axis_size(a) for a in (PLANE, LINE, "core"))
    total = jnp.float32(rows * plane * line)
    block = width // plane
    share = block // line
    sketch = lax.dot_general(
        tokens_x, test_matrix, (((1,), (1,)), ((), ())), preferred_element_type=jnp.float32
    )
    high, low = in_two(sketch)
    blocks = jnp.swapaxes(tokens_x.reshape(rows, plane, block), 0, 1)
    spare = -(block + 2 * columns) % LANES
    own = jnp.pad(jnp.concatenate([high, low], 1), ((0, 0), (0, spare)))
    own = jnp.broadcast_to(own, (plane, *own.shape))
    mixed = exchanged(jnp.concatenate([blocks, own], 2), PLANE).reshape(plane * rows, -1)
    tokens = mixed[:, :block]
    high = mixed[:, block : block + columns]
    low = mixed[:, block + columns : block + 2 * columns]
    gram = gram_of(high, low, total)
    cross = over_tokens(tokens, high)
    part = columns // line
    sent = jnp.concatenate(
        [
            cross.reshape(line, share, columns),
            jnp.pad(gram.reshape(line, part, columns), ((0, 0), (0, GROUP - part), (0, 0))),
        ],
        1,
    )
    whole = from_everyone(jnp.sum(exchanged(sent, LINE), 0), LINE)
    cross = whole[:, :share].reshape(block, columns)
    gram_one = whole[:, share : share + part].reshape(columns, columns)
    middle = solved(cross, inverse_factor(gram_one)).astype(jnp.bfloat16)
    power = jnp.dot(tokens, middle, preferred_element_type=jnp.float32)
    power = jnp.sum(exchanged(power.reshape(plane, rows, columns), PLANE), 0)
    powers = from_everyone(power, PLANE).reshape(plane * rows, columns)
    high, low = in_two(powers)
    gram = gram_of(high, low, total)
    cross_two = over_tokens(tokens, high)
    own = lax.axis_index("core")
    both = lax.all_gather(jnp.concatenate([cross_two, gram]), "core")
    both = both[0] + both[1]
    lines = both[:block].reshape(line // pair, pair, share, columns)
    half = both[block:].reshape(pair, -1, columns)
    lines = lax.dynamic_index_in_dim(lines, own, 1, False)
    half = lax.dynamic_index_in_dim(half, own, 0, False)
    half = jnp.broadcast_to(half, (line // pair, *half.shape))
    own = jnp.sum(exchanged(jnp.concatenate([lines, half], 1), "z"), 0)
    cross_two = own[:share]
    gram_two = lax.all_gather(own[share:], "core", axis=0, tiled=True)
    inverse_two = inverse_factor(gram_two)
    basis = solved(power, inverse_two)
    projected = solved(cross_two, inverse_two) / jnp.sqrt(total)
    return (basis, projected)


def solution(mesh):
    finer = Mesh(mesh.devices.reshape(4, 4, 8, mesh.shape["sub"]), EVERY)
    return jax.shard_map(
        on_device,
        mesh=finer,
        in_specs=(P(EVERY, None), P()),
        out_specs=(P(EVERY, None), P(EVERY, None)),
        check_vma=False,
    )
```

```python
import functools

import jax
import jax.numpy as jnp
from jax import lax
from jax.experimental import pallas as pl
from jax.experimental.pallas import tpu as pltpu
from jax.sharding import Mesh
from jax.sharding import PartitionSpec as P

PLANE = ("x", "y")
LINE = ("z", "core")
EVERY = ("x", "y", "z", "core")
GROUP = 8
LANES = 128


def exchanged(array, axes):
    return lax.all_to_all(array, axes, 0, 0, tiled=True)


def from_everyone(array, axes):
    return exchanged(jnp.broadcast_to(array, (lax.axis_size(axes), *array.shape)), axes)


def invert_factor(gram, inverse):
    size = gram.shape[0]
    shape = (GROUP, size)
    lane = lax.broadcasted_iota(jnp.int32, shape, 1)
    row = lax.broadcasted_iota(jnp.int32, shape, 0)

    def column(value, at):
        return jnp.broadcast_to(value[:, at : at + 1], shape)

    def line(value, at):
        return jnp.broadcast_to(value[at : at + 1], shape)

    groups = [gram[pl.ds(first, GROUP), :] for first in range(0, size, GROUP)]
    for at, own in enumerate(groups):
        first = at * GROUP
        columns = [column(own, first + k) for k in range(GROUP)]
        pivots = jnp.ones(shape, jnp.float32)
        lines, scales, uppers = [], [], {}
        for k in range(GROUP):
            pivot = line(columns[k], k)
            scale = 1.0 / pivot
            pivots = jnp.where(row == k, pivot, pivots)
            factor = jnp.where(row > k, columns[k] * scale, 0.0)
            own = jnp.where((lane == first + k) & (row >= k), jnp.where(row == k, 1.0, 0.0), own)
            lines.append(line(own, k))
            scales.append(scale)
            own = own - factor * lines[k]
            lines[k] = jnp.where((lane > first + k) & (lane < first + GROUP), 0.0, lines[k])
            for j in range(k + 1, GROUP):
                uppers[k, j] = line(columns[j], k)
                columns[j] = columns[j] - factor * uppers[k, j]
        inverse[pl.ds(first, GROUP), :] = jnp.where(
            lane <= first + row, own * lax.rsqrt(pivots), 0.0
        )
        inside = (lane >= first) & (lane < first + GROUP)
        for later in range(at + 1, len(groups)):
            value = groups[later]
            columns = [column(value, first + k) for k in range(GROUP)]
            value = jnp.where(inside, 0.0, value)
            for k in range(GROUP):
                factor = columns[k] * scales[k]
                value = value - factor * lines[k]
                for j in range(k + 1, GROUP):
                    columns[j] = columns[j] - factor * uppers[k, j]
            groups[later] = value

def times(left, right, right_dim):
    return lax.dot_general(
        left,
        right,
        (((1,), (right_dim,)), ((), ())),
        precision=lax.Precision.HIGHEST,
        preferred_element_type=jnp.float32,
    )


def middle_kernel(gram, cross, middle, inverse):
    invert_factor(gram, inverse)
    middle[...] = times(inverse[...], cross[...], 0).astype(jnp.bfloat16)


def outputs_kernel(gram, power, cross_two, basis, projected, inverse, *, scale):
    invert_factor(gram, inverse)
    basis[...] = times(power[...], inverse[...], 1)
    projected[...] = times(cross_two[...], inverse[...], 1) * scale


def near(*arrays):
    return [pltpu.with_memory_space_constraint(a, pltpu.VMEM) for a in arrays]


def middle_of(gram, cross):
    return pl.pallas_call(
        middle_kernel,
        out_shape=pltpu.VMEM(cross.shape, jnp.bfloat16),
        scratch_shapes=[pltpu.VMEM(gram.shape, jnp.float32)],
    )(*near(gram, cross))


def outputs_of(gram, power, cross_two, total):
    return pl.pallas_call(
        functools.partial(outputs_kernel, scale=float(total) ** -0.5),
        out_shape=[
            jax.ShapeDtypeStruct(power.shape, jnp.float32),
            jax.ShapeDtypeStruct(cross_two.shape, jnp.float32),
        ],
        scratch_shapes=[pltpu.VMEM(gram.shape, jnp.float32)],
    )(*near(gram, power, cross_two))


def over_tokens(left, right):
    return lax.dot_general(
        left, right, (((0,), (0,)), ((), ())), preferred_element_type=jnp.float32
    )


def in_two(array):
    high = lax.reduce_precision(array, 8, 7)
    return high.astype(jnp.bfloat16), (array - high).astype(jnp.bfloat16)


def in_three(array):
    high = lax.reduce_precision(array, 8, 7)
    rest = array - high
    middle = lax.reduce_precision(rest, 8, 7)
    return [part.astype(jnp.bfloat16) for part in (high, middle, rest - middle)]


def gram_of(high, low, total):
    product = over_tokens(high, high) + over_tokens(low, high)
    return (product + product.T) / (2.0 * total)


def on_device(tokens_x, test_matrix):
    rows, width = tokens_x.shape
    columns = test_matrix.shape[0]
    plane, line, pair = (lax.axis_size(a) for a in (PLANE, LINE, "core"))
    total = rows * plane * line
    block = width // plane
    share = block // line
    sketch = lax.dot_general(
        tokens_x, test_matrix, (((1,), (1,)), ((), ())), preferred_element_type=jnp.float32
    )
    high, low = in_two(sketch)
    blocks = jnp.swapaxes(tokens_x.reshape(rows, plane, block), 0, 1)
    spare = -(block + 2 * columns) % LANES
    own = jnp.pad(jnp.concatenate([high, low], 1), ((0, 0), (0, spare)))
    own = jnp.broadcast_to(own, (plane, *own.shape))
    mixed = exchanged(jnp.concatenate([blocks, own], 2), PLANE).reshape(plane * rows, -1)
    tokens = mixed[:, :block]
    high = mixed[:, block : block + columns]
    low = mixed[:, block + columns : block + 2 * columns]
    gram = gram_of(high, low, total)
    own = lax.axis_index("core")
    cross = over_tokens(high, tokens)
    both = jnp.pad(jnp.concatenate([cross, gram], 1), ((0, 0), (0, -columns % LANES)))
    both = lax.all_gather(both.reshape(pair, columns // pair, -1), "core")
    half = lax.dynamic_index_in_dim(both[0] + both[1], own, 0, False)
    cross = half[:, :block].astype(jnp.bfloat16)
    sent = from_everyone(jnp.concatenate([cross, *in_three(half[:, block:])], 1), "z")
    cross = sent[:, :, :block].astype(jnp.float32)
    gram = sum(part.astype(jnp.float32) for part in jnp.split(sent[:, :, block:], 3, 2))
    half = jnp.sum(jnp.concatenate([cross, gram], 2), 0)
    whole = lax.all_gather(half, "core", axis=0, tiled=True)
    middle = middle_of(whole[:, block : block + columns], whole[:, :block])
    power = lax.dot_general(
        tokens, middle, (((1,), (1,)), ((), ())), preferred_element_type=jnp.float32
    )
    power = jnp.sum(exchanged(power.reshape(plane, rows, columns), PLANE), 0)
    powers = from_everyone(power, PLANE).reshape(plane * rows, columns)
    high, low = in_two(powers)
    gram = gram_of(high, low, total)
    cross_two = over_tokens(tokens, high)
    both = lax.all_gather(jnp.concatenate([cross_two, gram]), "core")
    both = both[0] + both[1]
    lines = both[:block].reshape(line // pair, pair, share, columns)
    half = both[block:].reshape(pair, -1, columns)
    lines = lax.dynamic_index_in_dim(lines, own, 1, False)
    half = lax.dynamic_index_in_dim(half, own, 0, False)
    half = jnp.broadcast_to(half, (line // pair, *half.shape))
    summed = jnp.sum(exchanged(jnp.concatenate([lines, half], 1), "z"), 0)
    gram_two = lax.all_gather(summed[share:], "core", axis=0, tiled=True)
    return tuple(outputs_of(gram_two, power, summed[:share], total))


def solution(mesh):
    finer = Mesh(mesh.devices.reshape(4, 4, 8, mesh.shape["sub"]), EVERY)
    return jax.shard_map(
        on_device,
        mesh=finer,
        in_specs=(P(EVERY, None), P()),
        out_specs=(P(EVERY, None), P(EVERY, None)),
        check_vma=False,
    )
```

```python
import functools

import jax
import jax.numpy as jnp
from jax import lax
from jax.experimental import pallas as pl
from jax.experimental.pallas import tpu as pltpu
from jax.sharding import Mesh
from jax.sharding import PartitionSpec as P

PLANE = ("x", "y")
LINE = ("z", "core")
EVERY = ("x", "y", "z", "core")
GROUP = 8
LANES = 128
PIECES = 4


def exchanged(array, axes):
    return lax.all_to_all(array, axes, 0, 0, tiled=True)


def from_everyone(array, axes):
    return exchanged(jnp.broadcast_to(array, (lax.axis_size(axes), *array.shape)), axes)


def invert_factor(gram, inverse):
    size = inverse.shape[0]
    shape = (GROUP, size)
    lane = lax.broadcasted_iota(jnp.int32, shape, 1)
    row = lax.broadcasted_iota(jnp.int32, shape, 0)

    def column(value, at):
        return jnp.broadcast_to(value[:, at : at + 1], shape)

    def line(value, at):
        return jnp.broadcast_to(value[at : at + 1], shape)

    groups = [gram[first : first + GROUP, :size] for first in range(0, size, GROUP)]
    for at, own in enumerate(groups):
        first = at * GROUP
        columns = [column(own, first + k) for k in range(GROUP)]
        pivots = jnp.ones(shape, jnp.float32)
        lines, scales, uppers = [], [], {}
        for k in range(GROUP):
            pivot = line(columns[k], k)
            scale = 1.0 / pivot
            pivots = jnp.where(row == k, pivot, pivots)
            factor = jnp.where(row > k, columns[k] * scale, 0.0)
            own = jnp.where((lane == first + k) & (row >= k), jnp.where(row == k, 1.0, 0.0), own)
            lines.append(line(own, k))
            scales.append(scale)
            own = own - factor * lines[k]
            lines[k] = jnp.where((lane > first + k) & (lane < first + GROUP), 0.0, lines[k])
            for j in range(k + 1, GROUP):
                uppers[k, j] = line(columns[j], k)
                columns[j] = columns[j] - factor * uppers[k, j]
        inverse[pl.ds(first, GROUP), :] = jnp.where(
            lane <= first + row, own * lax.rsqrt(pivots), 0.0
        )
        inside = (lane >= first) & (lane < first + GROUP)
        for later in range(at + 1, len(groups)):
            value = groups[later]
            columns = [column(value, first + k) for k in range(GROUP)]
            value = jnp.where(inside, 0.0, value)
            for k in range(GROUP):
                factor = columns[k] * scales[k]
                value = value - factor * lines[k]
                for j in range(k + 1, GROUP):
                    columns[j] = columns[j] - factor * uppers[k, j]
            groups[later] = value

def times(left, right, right_dim):
    return lax.dot_general(
        left,
        right,
        (((1,), (right_dim,)), ((), ())),
        precision=lax.Precision.HIGHEST,
        preferred_element_type=jnp.float32,
    )


def middle_kernel(summed, middle, inverse):
    block = middle.shape[1]
    invert_factor(summed[:, block:], inverse)
    middle[...] = times(inverse[...], summed[:, :block], 0).astype(jnp.bfloat16)


def outputs_kernel(parts, power, basis, projected, inverse, *, scale):
    columns = power.shape[1]
    summed = parts[0]
    for at in range(1, parts.shape[0]):
        summed = summed + parts[at]
    invert_factor(summed, inverse)
    basis[...] = times(power[...], inverse[...], 1)
    own = summed[:, columns : columns + projected.shape[0]]
    projected[...] = times(inverse[...], own, 0).T * scale


def near(*arrays):
    return [pltpu.with_memory_space_constraint(a, pltpu.VMEM) for a in arrays]


def packed_kernel(_, tokens, test_matrix, sent, left, right, signals):
    count, rows, wide = sent.shape
    block = tokens.shape[1] // count
    pieces = signals.shape[1]
    each = count // pieces
    piece = each * block
    spans = [pl.ds(at * piece, piece) for at in range(pieces)]
    copies = [
        [
            pltpu.make_async_copy(source.at[:, spans[at]], held.at[:, spans[at]], signal.at[at])
            for at in range(pieces)
        ]
        for source, held, signal in (
            (tokens, left, signals.at[0]),
            (test_matrix, right, signals.at[1]),
        )
    ]
    for pair in zip(*copies, strict=True):
        for copy in pair:
            copy.start()
    sketch = jnp.zeros((rows, test_matrix.shape[0]), jnp.float32)
    for at, pair in enumerate(zip(*copies, strict=True)):
        for copy in pair:
            copy.wait()
        sketch += lax.dot_general(
            left[:, spans[at]],
            right[:, spans[at]],
            (((1,), (1,)), ((), ())),
            preferred_element_type=jnp.float32,
        )
        for to in range(at * each, (at + 1) * each):
            sent[to, :, :block] = left[:, to * block : (to + 1) * block]
    high = sketch.astype(jnp.bfloat16)
    low = (sketch - high.astype(jnp.float32)).astype(jnp.bfloat16)
    spare = jnp.zeros((rows, wide - block - 2 * sketch.shape[1]), jnp.bfloat16)
    tail = jnp.concatenate([high, low, spare], 1)
    for to in range(count):
        sent[to, :, block:] = tail


def packed(own, tokens, test_matrix, count):
    rows, width = tokens.shape
    wide = width // count + 2 * test_matrix.shape[0]
    return pl.pallas_call(
        packed_kernel,
        in_specs=[
            pl.BlockSpec(memory_space=pltpu.SMEM),
            pl.BlockSpec(memory_space=pl.ANY),
            pl.BlockSpec(memory_space=pl.ANY),
        ],
        out_shape=pltpu.VMEM((count, rows, wide + -wide % LANES), jnp.bfloat16),
        scratch_shapes=[
            pltpu.VMEM(tokens.shape, tokens.dtype),
            pltpu.VMEM(test_matrix.shape, test_matrix.dtype),
            pltpu.SemaphoreType.DMA((2, PIECES)),
        ],
    )(own, tokens, test_matrix)


def over_rows(left, right):
    return lax.dot_general(
        left, right, (((0,), (0,)), ((), ())), preferred_element_type=jnp.float32
    )


def cross_kernel(mixed, both, *, block, scale):
    columns = both.shape[0]
    high = mixed[:, block : block + columns]
    product = over_rows(high, mixed[...])
    gram = product[:, block : block + columns] + product[:, block + columns : block + 2 * columns]
    spare = jnp.zeros((columns, both.shape[1] - block - columns), jnp.float32)
    both[:, :block] = product[:, :block]
    both[:, block:] = jnp.concatenate([(gram + gram.T) * scale, spare], 1)


def cross_of(mixed, columns, block, total):
    return pl.pallas_call(
        functools.partial(cross_kernel, block=block, scale=0.5 / total),
        out_shape=pltpu.VMEM((columns, block + columns + -columns % LANES), jnp.float32),
    )(*near(mixed))


def cross_two_kernel(mixed, powers, both, *, block, scale):
    columns = both.shape[0]
    exact = powers[...]
    high = exact.astype(jnp.bfloat16)
    low = (exact - high.astype(jnp.float32)).astype(jnp.bfloat16)
    gram = over_rows(high, high) + over_rows(high, low)
    spare = jnp.zeros((columns, both.shape[1] - block - columns), jnp.float32)
    both[:, :block] = over_rows(high, mixed[:, :block])
    both[:, block:] = jnp.concatenate([(gram + gram.T) * scale, spare], 1)


def cross_two_of(mixed, powers, block, total):
    columns = powers.shape[1]
    return pl.pallas_call(
        functools.partial(cross_two_kernel, block=block, scale=0.5 / total),
        out_shape=pltpu.VMEM((columns, block + columns + -columns % LANES), jnp.float32),
    )(*near(mixed, powers))


def middle_of(summed, block):
    columns = summed.shape[0]
    return pl.pallas_call(
        middle_kernel,
        out_shape=pltpu.VMEM((columns, block), jnp.bfloat16),
        scratch_shapes=[pltpu.VMEM((columns, columns), jnp.float32)],
    )(*near(summed))


def outputs_of(parts, power, share, total):
    columns = power.shape[1]
    return pl.pallas_call(
        functools.partial(outputs_kernel, scale=total**-0.5),
        out_shape=[
            jax.ShapeDtypeStruct(power.shape, jnp.float32),
            jax.ShapeDtypeStruct((share, columns), jnp.float32),
        ],
        scratch_shapes=[pltpu.VMEM((columns, columns), jnp.float32)],
    )(*near(parts, power))


def spread_kernel(own, both, sent, *, block, share):
    columns = both.shape[1]
    summed = both[0] + both[1]
    gram = summed[:, block : block + columns]
    lines = summed[:, :block]
    lines = jnp.where(own[0] == 0, lines, pltpu.roll(lines, block - share, 1))
    spare = jnp.zeros((columns, sent.shape[2] - columns - share), jnp.float32)
    for to in range(sent.shape[0]):
        first = 2 * share * to
        sent[to] = jnp.concatenate([gram, lines[:, first : first + share], spare], 1)


def spread(both, own, line, share):
    columns = both.shape[1]
    lanes = columns + share
    return pl.pallas_call(
        functools.partial(spread_kernel, block=line * share, share=share),
        in_specs=[pl.BlockSpec(memory_space=pltpu.SMEM), pl.BlockSpec()],
        out_shape=pltpu.VMEM((line // 2, columns, lanes + -lanes % LANES), jnp.float32),
    )(own, *near(both))


def in_three(array):
    high = lax.reduce_precision(array, 8, 7)
    rest = array - high
    middle = lax.reduce_precision(rest, 8, 7)
    return [part.astype(jnp.bfloat16) for part in (high, middle, rest - middle)]


def on_device(tokens_x, test_matrix):
    rows, width = tokens_x.shape
    columns = test_matrix.shape[0]
    plane, line, pair = (lax.axis_size(a) for a in (PLANE, LINE, "core"))
    total = rows * plane * line
    block = width // plane
    share = block // line
    own = lax.axis_index("core").reshape(1)
    sent = packed(own, tokens_x, test_matrix, plane)
    mixed = exchanged(sent, PLANE).reshape(plane * rows, -1)
    both = cross_of(mixed, columns, block, total)
    both = lax.all_gather(both.reshape(pair, columns // pair, -1), "core")
    half = lax.dynamic_index_in_dim(both[0] + both[1], own[0], 0, False)
    cross = half[:, :block].astype(jnp.bfloat16)
    sent = from_everyone(jnp.concatenate([cross, *in_three(half[:, block:])], 1), "z")
    cross = sent[:, :, :block].astype(jnp.float32)
    gram = sum(part.astype(jnp.float32) for part in jnp.split(sent[:, :, block:], 3, 2))
    half = jnp.sum(jnp.concatenate([cross, gram], 2), 0)
    whole = lax.all_gather(half, "core", axis=0, tiled=True)
    middle = middle_of(whole, block)
    power = lax.dot_general(
        mixed[:, :block],
        middle,
        (((1,), (1,)), ((), ())),
        preferred_element_type=jnp.float32,
    )
    power = jnp.sum(exchanged(power.reshape(plane, rows, columns), PLANE), 0)
    powers = from_everyone(power, PLANE).reshape(plane * rows, columns)
    both = lax.all_gather(cross_two_of(mixed, powers, block, total), "core")
    parts = exchanged(spread(both, own, line, share), "z")
    return tuple(outputs_of(parts, power, share, total))


def solution(mesh):
    finer = Mesh(mesh.devices.reshape(4, 4, 8, mesh.shape["sub"]), EVERY)
    return jax.shard_map(
        on_device,
        mesh=finer,
        in_specs=(P(EVERY, None), P()),
        out_specs=(P(EVERY, None), P(EVERY, None)),
        check_vma=False,
    )
```

```python
import functools

import jax
import jax.numpy as jnp
from jax import lax
from jax.experimental import pallas as pl
from jax.experimental.pallas import tpu as pltpu
from jax.sharding import Mesh
from jax.sharding import PartitionSpec as P

PLANE = ("x", "y")
LINE = ("z", "core")
EVERY = ("x", "y", "z", "core")
GROUP = 8
LANES = 128
PIECES = 4


def exchanged(array, axes):
    return lax.all_to_all(array, axes, 0, 0, tiled=True)


def traded(array):
    return lax.ppermute(array, "core", [(0, 1), (1, 0)])


def in_two(array):
    high = array.astype(jnp.bfloat16)
    return high, (array - high.astype(jnp.float32)).astype(jnp.bfloat16)


def in_three(array):
    high = array.astype(jnp.bfloat16)
    rest = array - high.astype(jnp.float32)
    middle, low = in_two(rest)
    return high, middle, low


def invert_factor(gram, inverse):
    size = inverse.shape[0]
    shape = (GROUP, size)
    lane = lax.broadcasted_iota(jnp.int32, shape, 1)
    row = lax.broadcasted_iota(jnp.int32, shape, 0)

    def column(value, at):
        return jnp.broadcast_to(value[:, at : at + 1], shape)

    def line(value, at):
        return jnp.broadcast_to(value[at : at + 1], shape)

    groups = [gram[first : first + GROUP, :size] for first in range(0, size, GROUP)]
    for at, own in enumerate(groups):
        first = at * GROUP
        columns = [column(own, first + k) for k in range(GROUP)]
        pivots = jnp.ones(shape, jnp.float32)
        lines, scales, uppers = [], [], {}
        for k in range(GROUP):
            pivot = line(columns[k], k)
            scale = 1.0 / pivot
            pivots = jnp.where(row == k, pivot, pivots)
            factor = jnp.where(row > k, columns[k] * scale, 0.0)
            own = jnp.where((lane == first + k) & (row >= k), jnp.where(row == k, 1.0, 0.0), own)
            lines.append(line(own, k))
            scales.append(scale)
            own = own - factor * lines[k]
            lines[k] = jnp.where((lane > first + k) & (lane < first + GROUP), 0.0, lines[k])
            for j in range(k + 1, GROUP):
                uppers[k, j] = line(columns[j], k)
                columns[j] = columns[j] - factor * uppers[k, j]
        inverse[pl.ds(first, GROUP), :] = jnp.where(
            lane <= first + row, own * lax.rsqrt(pivots), 0.0
        )
        inside = (lane >= first) & (lane < first + GROUP)
        for later in range(at + 1, len(groups)):
            value = groups[later]
            columns = [column(value, first + k) for k in range(GROUP)]
            value = jnp.where(inside, 0.0, value)
            for k in range(GROUP):
                factor = columns[k] * scales[k]
                value = value - factor * lines[k]
                for j in range(k + 1, GROUP):
                    columns[j] = columns[j] - factor * uppers[k, j]
            groups[later] = value

def times(left, right, right_dim):
    return lax.dot_general(
        left,
        right,
        (((1,), (right_dim,)), ((), ())),
        precision=lax.Precision.HIGHEST,
        preferred_element_type=jnp.float32,
    )


def over_rows(left, right):
    return lax.dot_general(
        left, right, (((0,), (0,)), ((), ())), preferred_element_type=jnp.float32
    )


def corners(size):
    shape = (size, size)
    return lax.broadcasted_iota(jnp.int32, shape, 0), lax.broadcasted_iota(jnp.int32, shape, 1)


def halves_of(gram):
    size = gram.shape[0] // 2
    row, column = corners(size)
    last = gram[size:, size:]
    mixed = jnp.where(row >= column, gram[:size, :size], last)
    diagonal = jnp.sum(jnp.where(row == column, last, 0.0), 1, keepdims=True)
    return gram[size:, :size], mixed, diagonal


def gram_from(square, mixed, diagonal):
    row, column = corners(square.shape[0])
    under = jnp.where(row > column, mixed, 0.0)
    over = jnp.where(row < column, mixed, 0.0)
    first = under + under.T + jnp.where(row == column, mixed, 0.0)
    last = over + over.T + jnp.where(row == column, diagonal, 0.0)
    top = jnp.concatenate([first, square.T], 1)
    return jnp.concatenate([top, jnp.concatenate([square, last], 1)], 0)


def widened(array, lanes=LANES):
    rows, width = array.shape
    return jnp.concatenate([array, jnp.zeros((rows, lanes - width), array.dtype)], 1)


def folded(square, diagonal):
    both = jnp.concatenate([square, diagonal], 1)
    rows = both.shape[0] // 2
    return widened(jnp.concatenate([both[:rows], both[rows:]], 1))


def unfolded(array, size):
    both = jnp.concatenate([array[:, : size + 1], array[:, size + 1 : 2 * size + 2]], 0)
    return both[:, :size], both[:, size:]


def dense(array):
    width = array.shape[1]
    spare = LANES - width
    rows = array.shape[0] * width // LANES
    rest = array[rows:]
    side = jnp.concatenate([rest[:, at : at + spare] for at in range(0, width, spare)], 0)
    return jnp.concatenate([array[:rows], side], 1)


def undense(array, width):
    spare = LANES - width
    side = array[:, width:]
    each = array.shape[0] * spare // width
    parts = [side[at : at + each] for at in range(0, side.shape[0], each)]
    return jnp.concatenate([array[:, :width], jnp.concatenate(parts, 1)], 0)


def near(*arrays):
    return [pltpu.with_memory_space_constraint(a, pltpu.VMEM) for a in arrays]


def whole(count):
    return [pl.BlockSpec(memory_space=pltpu.SMEM)] + [pl.BlockSpec()] * count


def packed_kernel(_, tokens, test_matrix, sent, left, right, signals):
    count, _, block = sent.shape
    rows = tokens.shape[0]
    pieces = signals.shape[1]
    each = count // pieces
    piece = each * block
    spans = [pl.ds(at * piece, piece) for at in range(pieces)]
    copies = [
        [
            pltpu.make_async_copy(source.at[:, spans[at]], held.at[:, spans[at]], signal.at[at])
            for at in range(pieces)
        ]
        for source, held, signal in (
            (tokens, left, signals.at[0]),
            (test_matrix, right, signals.at[1]),
        )
    ]
    for pair in zip(*copies, strict=True):
        for copy in pair:
            copy.start()
    sketch = jnp.zeros((rows, test_matrix.shape[0]), jnp.float32)
    for at, pair in enumerate(zip(*copies, strict=True)):
        for copy in pair:
            copy.wait()
        sketch += lax.dot_general(
            left[:, spans[at]],
            right[:, spans[at]],
            (((1,), (1,)), ((), ())),
            preferred_element_type=jnp.float32,
        )
        for to in range(at * each, (at + 1) * each):
            sent[to, :rows] = left[:, to * block : (to + 1) * block]
    high, low = in_two(sketch)
    half = rows // 2
    side = jnp.concatenate([high[:half], low[:half], high[half:], low[half:]], 1)
    for to in range(count):
        sent[to, rows:] = side


def packed(own, tokens, test_matrix, count):
    rows, width = tokens.shape
    return pl.pallas_call(
        packed_kernel,
        in_specs=[
            pl.BlockSpec(memory_space=pltpu.SMEM),
            pl.BlockSpec(memory_space=pl.ANY),
            pl.BlockSpec(memory_space=pl.ANY),
        ],
        out_shape=pltpu.VMEM((count, rows + rows // 2, width // count), jnp.bfloat16),
        scratch_shapes=[
            pltpu.VMEM(tokens.shape, tokens.dtype),
            pltpu.VMEM(test_matrix.shape, test_matrix.dtype),
            pltpu.SemaphoreType.DMA((2, PIECES)),
        ],
    )(own, tokens, test_matrix)


def chosen(own, zero, one):
    return jnp.where(own[0] == 0, zero, one), jnp.where(own[0] == 0, one, zero)


def cross_kernel(own, mixed, keep, give, *, rows, scale):
    count, tall, block = mixed.shape
    columns = block // 4
    size = columns // 2
    half = rows // 2
    flat = (count * half, block)
    side = mixed[:, rows:].reshape(flat)
    cross = over_rows(side[:, :columns], mixed[:, :half].reshape(flat))
    skip = 2 * columns // LANES * LANES
    start = 2 * columns - skip
    again = over_rows(side[:, skip:], mixed[:, half:rows].reshape(flat))
    cross += again[start : start + columns]
    square = over_rows(side, side)
    gram = jnp.zeros((columns, columns), jnp.float32)
    for first in (0, 2 * columns):
        own_rows = square[first : first + columns]
        gram += own_rows[:, first : first + columns]
        gram += own_rows[:, first + columns : first + 2 * columns]
    lower, both, diagonal = halves_of((gram + gram.T) * scale)
    grams = folded(lower, jnp.zeros_like(diagonal)), folded(both, diagonal)
    keep[:size], give[:size] = chosen(own, cross[:size], cross[size:])
    keep[size:], give[size:] = (widened(a, block) for a in chosen(own, *grams))


def cross_of(own, mixed, rows, total):
    count, _, block = mixed.shape
    size = block // 8
    shape = pltpu.VMEM((size + size // 2, block), jnp.float32)
    return pl.pallas_call(
        functools.partial(cross_kernel, rows=rows, scale=0.5 / total),
        in_specs=whole(1),
        out_shape=[shape, shape],
    )(own, *near(mixed))


def spread_kernel(keep, got, sent, *, size):
    cross = (keep[:size] + got[:size]).astype(jnp.bfloat16)
    gram = keep[size:, :LANES] + got[size:, :LANES]
    parts = jnp.concatenate(in_three(gram), 1)
    for to in range(sent.shape[0]):
        sent[to, :size] = cross
        sent[to, size:] = parts


def spread(keep, got, count, size):
    return pl.pallas_call(
        functools.partial(spread_kernel, size=size),
        out_shape=pltpu.VMEM((count, *keep.shape), jnp.bfloat16),
    )(*near(keep, got))


def summed_kernel(parts, half, *, size):
    total = parts[0].astype(jnp.float32)
    for at in range(1, parts.shape[0]):
        total += parts[at].astype(jnp.float32)
    gram = total[size:]
    half[:size] = total[:size]
    gram = gram[:, :LANES] + gram[:, LANES : 2 * LANES] + gram[:, 2 * LANES :]
    half[size:] = widened(gram, half.shape[1])


def summed(parts, size):
    return pl.pallas_call(
        functools.partial(summed_kernel, size=size),
        out_shape=pltpu.VMEM(parts.shape[1:], jnp.float32),
    )(*near(parts))


def power_kernel(own, mixed, mine, other, sent, inverse, *, rows):
    count, _, block = mixed.shape
    size = inverse.shape[0] // 2
    first, second = chosen(own, mine[...], other[...])
    lower, _ = unfolded(first[size:, :LANES], size)
    both, diagonal = unfolded(second[size:, :LANES], size)
    invert_factor(gram_from(lower, both, diagonal), inverse)
    cross = jnp.concatenate([first[:size], second[:size]], 0)
    middle = times(inverse[...], cross, 0).astype(jnp.bfloat16)
    power = lax.dot_general(
        mixed[:, :rows].reshape(count * rows, block),
        middle,
        (((1,), (1,)), ((), ())),
        preferred_element_type=jnp.float32,
    )
    for to in range(count):
        sent[to] = dense(power[to * rows : (to + 1) * rows])


def power_of(own, mixed, mine, other, rows):
    count, _, block = mixed.shape
    columns = block // 4
    return pl.pallas_call(
        functools.partial(power_kernel, rows=rows),
        in_specs=whole(3),
        out_shape=pltpu.VMEM((count, rows * columns // LANES, LANES), jnp.float32),
        scratch_shapes=[pltpu.VMEM((columns, columns), jnp.float32)],
    )(own, *near(mixed, mine, other))


def cross_two_kernel(own, mixed, powers, keep, give, *, rows, scale):
    count, _, block = mixed.shape
    columns = block // 4
    size = columns // 2
    share = columns // 4
    exact = jnp.concatenate([undense(powers[at], columns) for at in range(count)], 0)
    high, low = in_two(exact)
    gram = over_rows(high, high) + over_rows(high, low)
    lower, both, diagonal = halves_of((gram + gram.T) * scale)
    keep[:size] = widened(jnp.concatenate([lower, both, diagonal], 1))
    give[:size] = keep[:size]
    lines = widened(over_rows(high, mixed[:, :rows].reshape(count * rows, block)).T)
    for at in range(block // (2 * share)):
        first = 2 * share * at
        pair = lines[first : first + share], lines[first + share : first + 2 * share]
        place = pl.ds(size + share * at, share)
        keep[place], give[place] = chosen(own, *pair)


def cross_two_of(own, mixed, powers, rows, total):
    _, _, block = mixed.shape
    shape = pltpu.VMEM((block // 8 + block // 2, LANES), jnp.float32)
    return pl.pallas_call(
        functools.partial(cross_two_kernel, rows=rows, scale=0.5 / total),
        in_specs=whole(2),
        out_shape=[shape, shape],
    )(own, *near(mixed, powers))


def spread_two_kernel(keep, got, sent, *, size):
    share = size // 2
    gram = keep[:size] + got[:size]
    for to in range(sent.shape[0]):
        place = pl.ds(size + share * to, share)
        sent[to, :size] = gram
        sent[to, size:] = keep[place] + got[place]


def spread_two(keep, got, count, size):
    return pl.pallas_call(
        functools.partial(spread_two_kernel, size=size),
        out_shape=pltpu.VMEM((count, size + size // 2, LANES), jnp.float32),
    )(*near(keep, got))


def outputs_kernel(parts, power, basis, projected, inverse, *, scale):
    columns = inverse.shape[0]
    size = columns // 2
    total = parts[0]
    for at in range(1, parts.shape[0]):
        total += parts[at]
    lower, both = total[:size, :size], total[:size, size:columns]
    invert_factor(gram_from(lower, both, total[:size, columns : columns + 1]), inverse)
    basis[...] = times(undense(power[...], columns), inverse[...], 1)
    projected[...] = times(total[size:, :columns], inverse[...], 1) * scale


def outputs_of(parts, power, rows, columns, total):
    return pl.pallas_call(
        functools.partial(outputs_kernel, scale=total**-0.5),
        out_shape=[
            jax.ShapeDtypeStruct((rows, columns), jnp.float32),
            jax.ShapeDtypeStruct((columns // 4, columns), jnp.float32),
        ],
        scratch_shapes=[pltpu.VMEM((columns, columns), jnp.float32)],
    )(*near(parts, power))


def on_device(tokens_x, test_matrix):
    rows = tokens_x.shape[0]
    columns = test_matrix.shape[0]
    size = columns // 2
    plane, line = lax.axis_size(PLANE), lax.axis_size("z")
    total = rows * lax.axis_size(EVERY)
    own = lax.axis_index("core").reshape(1)
    mixed = exchanged(packed(own, tokens_x, test_matrix, plane), PLANE)
    keep, give = cross_of(own, mixed, rows, total)
    half = summed(exchanged(spread(keep, traded(give), line, size), "z"), size)
    power = power_of(own, mixed, half, traded(half), rows)
    power = jnp.sum(exchanged(power, PLANE), 0)
    powers = exchanged(jnp.broadcast_to(power, (plane, *power.shape)), PLANE)
    keep, give = cross_two_of(own, mixed, powers, rows, total)
    parts = exchanged(spread_two(keep, traded(give), line, size), "z")
    return tuple(outputs_of(parts, power, rows, columns, total))


def solution(mesh):
    finer = Mesh(mesh.devices.reshape(4, 4, 8, mesh.shape["sub"]), EVERY)
    return jax.shard_map(
        on_device,
        mesh=finer,
        in_specs=(P(EVERY, None), P()),
        out_specs=(P(EVERY, None), P(EVERY, None)),
        check_vma=False,
    )
```
